32 devices in a mesh: row: 4 (over x, core), col: 8 (over z, y).
Axes of the slice: x: 2, y: 2, z: 4, core: 2. Of those that a mesh axis runs over, the one named last changes fastest.
Arguments:
- points: float32 [16, 8192], P(None, ('row', 'col')), may hold values from -6 to 6
- lengthscale: float32 [16], replicated, may hold values from 2 to 8
- signal: float32 [1], replicated, may hold values from 0.5 to 2
- noise: float32 [1], replicated, may hold values from 0.05 to 0.5
- targets: float32 [8192], P(('row', 'col')), may hold values from -12 to 12
- probe_bits: int32 [31, 8192], P(None, ('row', 'col')), may hold values from 0 to 1
Outputs:
- solution: float32 [32, 8192], P(None, ('row', 'col'))
- residual: float32 [32, 8192], P(None, ('row', 'col'))
The draws below stay inside these ranges and needn't reach their ends.
All inputs are finite; a program needn't handle non-finite values.
Results may differ from the reference program's by a relative error of at most 0.0013.
Values sent between devices are 32-bit elements; how exact they have to be, the bound alone decides.
A program may use at most 128 MiB of HBM per device.

```python
import math
import jax
import jax.numpy as jnp
from jax import lax

DIM = 16
PROBES = 31
ITERS = 3
N = 8192


def draw_targets(key, part):
    ramp = 1.0 + 2.0 * jnp.arange(N, dtype=jnp.float32) / N
    values = jnp.clip(jax.random.normal(key, (N,), jnp.float32), -4.0, 4.0)
    return values * ramp


def with_ends(array, stream_key, least, high):
    index_at = [jax.random.randint(jax.random.fold_in(stream_key, axis), (), 0, length) for axis, length in enumerate(array.shape)]
    longest = array.shape.index(max(array.shape))
    next_to = index_at[:longest] + [(index_at[longest] + 1) % array.shape[longest]] + index_at[longest + 1:]
    return array.at[tuple(index_at)].set(least).at[tuple(next_to)].set(high)


def level_of(stream_key, extent, split, low, high):
    def one(position, parts):
        draws = jax.random.uniform(jax.random.fold_in(jax.random.fold_in(stream_key, 6), position), (parts,), jnp.float32, low / len(split), high / len(split))
        return jnp.repeat(jnp.exp(draws), extent[position] // parts).reshape((-1,) + (1,) * (len(extent) - position - 1))

    factor_of = one(*split[0])
    for cut in split[1:]:
        factor_of = factor_of * one(*cut)
    return factor_of


def gaussian(stream_key, dims, spread, most, cuts=(), kind=jnp.bfloat16):
    values = jax.random.normal(stream_key, dims, jnp.float32) * spread
    if len(cuts) > 0:
        values = level_of(stream_key, dims, cuts, -0.22, 0.18) * values
    return jnp.clip(values, min=-most, max=most).astype(kind)


def setup_inputs(seed: int = 0) -> dict:
    keys = jax.random.split(jax.random.key(seed), 7)
    return {
        "points": gaussian(keys[0], (DIM, N), 1.0, 6.0, ((1, 32),), jnp.float32),
        "lengthscale": jnp.clip(jnp.exp(jax.random.uniform(keys[1], (DIM,), jnp.float32, math.log(2.0), math.log(8.0))), 2.0, 8.0),
        "signal": jnp.clip(jnp.exp(jax.random.uniform(keys[2], (1,), jnp.float32, math.log(0.5), math.log(2.0))), 0.5, 2.0),
        "noise": jnp.clip(jnp.exp(jax.random.uniform(keys[3], (1,), jnp.float32, math.log(0.05), math.log(0.5))), 0.05, 0.5),
        "targets": draw_targets(jax.random.fold_in(keys[6], 71), 0),
        "probe_bits": with_ends(jax.random.randint(keys[5], (PROBES, N), 0, 2), jax.random.fold_in(keys[5], 1), 0, 1).astype(jnp.int32),
    }


ROOT_FIVE = 5.0 ** 0.5

def matern_tile(row_scaled, col_scaled, signal_value):
    row_sq = lax.optimization_barrier(jnp.sum(row_scaled * row_scaled, axis=0))
    col_sq = lax.optimization_barrier(jnp.sum(col_scaled * col_scaled, axis=0))
    cross_term = lax.dot_general(row_scaled, col_scaled, (((0,), (0,)), ((), ())), precision=lax.Precision.HIGHEST, preferred_element_type=jnp.float32)
    dist_sq = jnp.maximum(row_sq[:, None] + col_sq[None, :] - 2.0 * cross_term, 0.0)
    radius = jnp.sqrt(dist_sq)
    return signal_value * (1.0 + ROOT_FIVE * radius + 5.0 / 3.0 * dist_sq) * jnp.exp(-ROOT_FIVE * radius)

def reference(points, lengthscale, signal, noise, targets, probe_bits):
    scaled = points / lengthscale[:, None]
    signs = 2.0 * probe_bits.astype(jnp.float32) - 1.0
    right_side = jnp.concatenate([targets[None, :], signs], axis=0)
    signal_value = signal[0]
    noise_value = noise[0]
    block_rows = min(2048, N)
    stacked = scaled.reshape(DIM, N // block_rows, block_rows).transpose(1, 0, 2)

    def operator(vectors):

        def one_block(row_block):
            kernel_tile = matern_tile(row_block, scaled, signal_value)
            return lax.dot_general(vectors, kernel_tile, (((1,), (1,)), ((), ())), precision=lax.Precision.HIGHEST, preferred_element_type=jnp.float32)
        pieces = lax.map(one_block, stacked)
        return pieces.transpose(1, 0, 2).reshape(vectors.shape[0], N) + noise_value * vectors
    solution = jnp.zeros_like(right_side)
    residual = right_side
    direction = right_side
    norm_now = lax.optimization_barrier(jnp.sum(residual * residual, axis=1))
    for step in range(ITERS):
        image = operator(direction)
        alpha = norm_now / lax.optimization_barrier(jnp.sum(direction * image, axis=1))
        solution = solution + alpha[:, None] * direction
        residual = residual - alpha[:, None] * image
        if step + 1 < ITERS:
            norm_next = lax.optimization_barrier(jnp.sum(residual * residual, axis=1))
            direction = residual + (norm_next / norm_now)[:, None] * direction
            norm_now = norm_next
    return (solution, residual)
```

```python
import functools
import math

import jax
import jax.numpy as jnp
from jax import lax
from jax.experimental import pallas as pl
from jax.experimental.pallas import tpu as pltpu
from jax.sharding import PartitionSpec as P

ITERS = 3
MESH = pl.DeviceIdType.MESH
LOG2E = math.log2(math.e)
POINT_SCALE = math.sqrt(5.0) * LOG2E
POINTS, RIGHT, IMAGE0, IMAGE1 = range(4)


def split(value, count):
    parts = []
    for _ in range(count):
        part = value.astype(jnp.bfloat16)
        parts.append(part)
        value = value - part.astype(jnp.float32)
    return parts


def norm_rows(points, first):
    norm = jnp.sum(points * points, axis=0, keepdims=True)
    n1, n2, n3 = [part.astype(jnp.float32) for part in split(norm, 3)]
    row = lax.broadcasted_iota(jnp.int32, points.shape, 0)
    base = 0 if first else 3
    ones = 3 - base
    rows = jnp.where((row >= ones) & (row < ones + 3), 1.0, 0.0)
    for place, part in enumerate((n1, n2, n3)):
        rows = jnp.where(row == base + place, part, rows)
    return rows.astype(jnp.bfloat16)


def left_stack(points):
    s1, s2, s3 = split(points, 3)
    return jnp.concatenate([s1, s1, s2, s2, s1, s3, norm_rows(points, True)], axis=0)


def right_stack(points):
    s1, s2, s3 = split(-2.0 * points, 3)
    return jnp.concatenate([s1, s2, s1, s2, s3, s1, norm_rows(points, False)], axis=0)


def kernel_body(
    rows, cols,
    points_ref, length_ref, signal_ref, noise_ref, targets_ref, bits_ref,
    solution_ref, residual_ref,
    pts, vec, im0, im1, halves, khi, klo, scal, own_right,
    send_peer, recv_peer, send_sib, recv_sib, send_scal, recv_scal,
):
    devices = rows * cols
    chips = devices // 2
    width = points_ref.shape[1]
    count = bits_ref.shape[0] + 1
    row = lax.axis_index("row")
    col = lax.axis_index("col")
    core = lax.rem(row, 2)
    me = row * cols + col
    chip = lax.div(row, 2) * cols + col
    buffers = (pts, vec, im0, im1)

    def slot_of(chip_index, core_index):
        high = lax.div(chip_index, cols)
        return (2 * high + core_index) * cols + lax.rem(chip_index, cols)

    def chip_id(chip_index, core_index):
        return (2 * lax.div(chip_index, cols) + core_index, lax.rem(chip_index, cols))

    def to_peer(phase, k):
        return pltpu.make_async_remote_copy(
            src_ref=buffers[phase].at[me],
            dst_ref=buffers[phase].at[me],
            send_sem=send_peer.at[phase, k],
            recv_sem=recv_peer.at[phase, k],
            device_id=chip_id(lax.rem(chip + k, chips), core),
            device_id_type=MESH,
        )

    def source(k):
        return lax.rem(chip + chips - k, chips)

    def to_sibling(phase, k):
        slot = slot_of(source(k), core)
        return pltpu.make_async_remote_copy(
            src_ref=buffers[phase].at[slot],
            dst_ref=buffers[phase].at[slot],
            send_sem=send_sib.at[phase, k],
            recv_sem=recv_sib.at[phase, k],
            device_id=(row + 1 - 2 * core, col),
            device_id_type=MESH,
        )

    def each(low, high, step):
        def run(k, carry):
            step(k)
            return carry

        lax.fori_loop(low, high, run, 0)

    def send_all(phase):
        each(1, chips, lambda k: to_peer(phase, k).start())
        to_sibling(phase, 0).start()

    def sent_all(phase):
        each(1, chips, lambda k: to_peer(phase, k).wait_send())
        each(0, chips, lambda k: to_sibling(phase, k).wait_send())

    def arrive_peer(phase, k):
        to_peer(phase, k).wait_recv()
        to_sibling(phase, k).start()

    diagonal = lax.broadcasted_iota(jnp.int32, (points_ref.shape[0],) * 2, 0) == lax.broadcasted_iota(
        jnp.int32, (points_ref.shape[0],) * 2, 1
    )
    length = jnp.sum(jnp.where(diagonal, length_ref[...], 0.0), axis=1, keepdims=True)
    mine = points_ref[...] / length * POINT_SCALE
    pts[me] = mine
    own_right[0:1, :] = targets_ref[...]
    own_right[1:count, :] = 2.0 * bits_ref[...].astype(jnp.float32) - 1.0
    vec[me] = own_right[...]

    barrier = pltpu.get_barrier_semaphore()

    def greet(k):
        other = lax.rem(me + k, devices)
        pl.semaphore_signal(
            barrier, inc=1, device_id=(lax.div(other, cols), lax.rem(other, cols)), device_id_type=MESH
        )

    each(1, devices, greet)
    pl.semaphore_wait(barrier, devices - 1)

    send_all(POINTS)
    send_all(RIGHT)

    signal = signal_ref[0]
    noise = noise_ref[0]
    c1 = signal * (1.0 / LOG2E)
    c2 = signal * (1.0 / (3.0 * LOG2E * LOG2E))
    across = right_stack(mine)

    def kernel_tile(slot):
        down = left_stack(pts[slot])
        square = lax.dot_general(
            down, across, (((0,), (0,)), ((), ())), preferred_element_type=jnp.float32
        )
        square = jnp.maximum(square, 1e-30)
        w = square * lax.rsqrt(square)
        tile = (signal + c1 * w + c2 * square) * jnp.exp2(-w)
        high = tile.astype(jnp.bfloat16)
        place = pl.ds(pl.multiple_of(slot * width, width), width)
        khi[place, :] = high
        klo[place, :] = (tile - high.astype(jnp.float32)).astype(jnp.bfloat16)

    kernel_tile(me)

    def peer_tile(k):
        arrive_peer(POINTS, k)
        kernel_tile(slot_of(source(k), core))

    each(1, chips, peer_tile)
    each(1, chips, lambda k: arrive_peer(RIGHT, k))

    def sibling_tile(k):
        to_sibling(POINTS, k).wait_recv()
        kernel_tile(slot_of(source(k), 1 - core))

    each(0, chips, sibling_tile)
    each(0, chips, lambda k: to_sibling(RIGHT, k).wait_recv())
    sent_all(POINTS)
    sent_all(RIGHT)

    zero = jnp.zeros((count, width), jnp.float32)

    def total(value):
        return jnp.sum(value, axis=1, keepdims=True)

    def put_halves(j, value):
        high = value.astype(jnp.bfloat16)
        place = pl.ds(pl.multiple_of(j * width, width), width)
        halves[0:count, place] = high
        halves[count : 2 * count, place] = (value - high.astype(jnp.float32)).astype(jnp.bfloat16)

    def first_pass(j, carry):
        value = vec[j]
        put_halves(j, value)
        return carry + value * value

    norm_now = total(lax.fori_loop(0, devices, first_pass, zero))

    def image():
        both = jnp.dot(halves[...], khi[...], preferred_element_type=jnp.float32)
        rest = jnp.dot(halves[0:count, :], klo[...], preferred_element_type=jnp.float32)
        return both[:count] + (both[count:] + rest) + noise * vec[me]

    solved = zero
    residuals = vec
    for step in range(ITERS - 1):
        phase = IMAGE0 + step
        images = buffers[phase]
        images[me] = image()
        send_all(phase)

        def from_peer(k, carry):
            arrive_peer(phase, k)
            slot = slot_of(source(k), core)
            return carry + vec[slot] * images[slot]

        def from_sibling(k, carry):
            to_sibling(phase, k).wait_recv()
            slot = slot_of(source(k), 1 - core)
            return carry + vec[slot] * images[slot]

        curved = vec[me] * images[me]
        curved = lax.fori_loop(1, chips, from_peer, curved)
        curved = lax.fori_loop(0, chips, from_sibling, curved)
        sent_all(phase)
        alpha = norm_now / total(curved)
        solved = solved + alpha * vec[me]

        def reduce_pass(j, carry):
            value = residuals[j] - alpha * images[j]
            images[j] = value
            return carry + value * value

        norm_next = total(lax.fori_loop(0, devices, reduce_pass, zero))
        beta = norm_next / norm_now
        norm_now = norm_next

        def turn_pass(j, carry):
            value = images[j] + beta * vec[j]
            vec[j] = value
            put_halves(j, value)
            return carry

        lax.fori_loop(0, devices, turn_pass, 0)
        residuals = images

    last = image()
    part = total(vec[me] * last)
    square_shape = (count, 128)
    on_diagonal = lax.broadcasted_iota(jnp.int32, square_shape, 0) == lax.broadcasted_iota(
        jnp.int32, square_shape, 1
    )
    line = jnp.sum(jnp.where(on_diagonal, part, 0.0), axis=0, keepdims=True)
    scal[me] = jnp.broadcast_to(line, scal.shape[1:])

    def scalar_copy(k):
        other = lax.rem(me + k, devices)
        return pltpu.make_async_remote_copy(
            src_ref=scal.at[me],
            dst_ref=scal.at[me],
            send_sem=send_scal.at[k],
            recv_sem=recv_scal.at[k],
            device_id=(lax.div(other, cols), lax.rem(other, cols)),
            device_id_type=MESH,
        )

    each(1, devices, lambda k: scalar_copy(k).start())
    each(1, devices, lambda k: scalar_copy(k).wait_recv())
    summed = lax.fori_loop(1, devices, lambda j, carry: carry + scal[j], scal[0])
    curved = total(jnp.where(on_diagonal, summed[0:1, :], 0.0))
    alpha = norm_now / curved
    solution_ref[...] = solved + alpha * vec[me]
    residual_ref[...] = residuals[me] - alpha * last
    each(1, devices, lambda k: scalar_copy(k).wait_send())


def solution(mesh):
    rows, cols = mesh.shape["row"], mesh.shape["col"]
    devices = rows * cols
    chips = devices // 2

    def body(points, lengthscale, signal, noise, targets, probe_bits):
        dims, width = points.shape
        count = probe_bits.shape[0] + 1
        block = jax.ShapeDtypeStruct((count, width), jnp.float32)
        vmem = pl.BlockSpec(memory_space=pltpu.VMEM)
        smem = pl.BlockSpec(memory_space=pltpu.SMEM)
        slots = pltpu.VMEM((devices, count, width), jnp.float32)
        return pl.pallas_call(
            functools.partial(kernel_body, rows, cols),
            out_shape=(block, block),
            in_specs=[vmem, vmem, smem, smem, vmem, vmem],
            out_specs=(vmem, vmem),
            scratch_shapes=[
                pltpu.VMEM((devices, dims, width), jnp.float32),
                slots,
                slots,
                slots,
                pltpu.VMEM((2 * count, devices * width), jnp.bfloat16),
                pltpu.VMEM((devices * width, width), jnp.bfloat16),
                pltpu.VMEM((devices * width, width), jnp.bfloat16),
                pltpu.VMEM((devices, 8, 128), jnp.float32),
                pltpu.VMEM((count, width), jnp.float32),
                pltpu.SemaphoreType.DMA((4, chips)),
                pltpu.SemaphoreType.DMA((4, chips)),
                pltpu.SemaphoreType.DMA((4, chips)),
                pltpu.SemaphoreType.DMA((4, chips)),
                pltpu.SemaphoreType.DMA((devices,)),
                pltpu.SemaphoreType.DMA((devices,)),
            ],
            compiler_params=pltpu.CompilerParams(
                collective_id=0, has_side_effects=True, vmem_limit_bytes=60 * 1024 * 1024
            ),
        )(points, lengthscale[None, :], signal, noise, targets[None, :], probe_bits)

    split_points = P(None, ("row", "col"))
    return jax.shard_map(
        body,
        mesh=mesh,
        in_specs=(split_points, P(), P(), P(), P(("row", "col")), split_points),
        out_specs=(split_points, split_points),
        check_vma=False,
    )
```

```python
import functools
import math

import jax
import jax.numpy as jnp
from jax import lax
from jax.experimental import pallas as pl
from jax.experimental.pallas import tpu as pltpu
from jax.sharding import PartitionSpec as P

ITERS = 3
MESH = pl.DeviceIdType.MESH
LOG2E = math.log2(math.e)
POINT_SCALE = math.sqrt(5.0) * LOG2E
POINTS, RIGHT, IMAGE0, IMAGE1 = range(4)


def split(value, count):
    parts = []
    for _ in range(count):
        part = value.astype(jnp.bfloat16)
        parts.append(part)
        value = value - part.astype(jnp.float32)
    return parts


def norm_rows(points, first):
    norm = jnp.sum(points * points, axis=0, keepdims=True)
    n1, n2, n3 = [part.astype(jnp.float32) for part in split(norm, 3)]
    row = lax.broadcasted_iota(jnp.int32, points.shape, 0)
    base = 0 if first else 3
    ones = 3 - base
    rows = jnp.where((row >= ones) & (row < ones + 3), 1.0, 0.0)
    for place, part in enumerate((n1, n2, n3)):
        rows = jnp.where(row == base + place, part, rows)
    return rows.astype(jnp.bfloat16)


def left_stack(points):
    s1, s2, s3 = split(points, 3)
    return jnp.concatenate([s1, s1, s2, s2, s1, s3, norm_rows(points, True)], axis=0)


def right_stack(points):
    s1, s2, s3 = split(-2.0 * points, 3)
    return jnp.concatenate([s1, s2, s1, s2, s3, s1, norm_rows(points, False)], axis=0)


def kernel_body(
    rows, cols,
    points_ref, length_ref, signal_ref, noise_ref, targets_ref, bits_ref,
    solution_ref, residual_ref,
    pts, vec, im0, im1, khi, klo, scal,
    send_peer, recv_peer, send_sib, recv_sib, send_scal, recv_scal,
):
    devices = rows * cols
    chips = devices // 2
    width = points_ref.shape[1]
    count = bits_ref.shape[0] + 1
    wide = rows // 2
    minor = 1
    while 4 * minor * minor <= cols:
        minor *= 2
    major = cols // minor
    chunk = major
    chunks = chips // chunk
    row = lax.axis_index("row")
    col = lax.axis_index("col")
    core = lax.rem(row, 2)
    x = lax.div(row, 2)
    z = lax.div(col, minor)
    y = lax.rem(col, minor)
    turned = core if wide == minor else 0
    first, second = wide, minor
    buffers = (pts, vec, im0, im1)

    def parts_of(k):
        return k % major, k // major % first, k // major // first

    def device_at(dz, df, ds):
        tx = lax.rem(x + df + turned * (ds - df), wide)
        ty = lax.rem(y + ds + turned * (df - ds), minor)
        tz = lax.rem(z + dz, major)
        return (2 * tx + core, tz * minor + ty)

    sibling = (row + 1 - 2 * core, col)

    def to_peer(phase, k):
        dz, df, ds = parts_of(k)
        if ds > 0:
            held, target = k - ds * first * major, (0, 0, ds)
        elif df > 0:
            held, target = dz, (0, df, 0)
        else:
            held, target = 0, (dz, 0, 0)
        return pltpu.make_async_remote_copy(
            src_ref=buffers[phase].at[held],
            dst_ref=buffers[phase].at[k],
            send_sem=send_peer.at[phase, k],
            recv_sem=recv_peer.at[phase, k],
            device_id=device_at(*target),
            device_id_type=MESH,
        )

    def to_sibling(phase, k):
        return pltpu.make_async_remote_copy(
            src_ref=buffers[phase].at[k],
            dst_ref=buffers[phase].at[chips + k],
            send_sem=send_sib.at[phase, k],
            recv_sem=recv_sib.at[phase, k],
            device_id=sibling,
            device_id_type=MESH,
        )

    def pass_on(phase, k):
        dz, df, ds = parts_of(k)
        if k == 0:
            for j in range(1, major):
                to_peer(phase, j).start()
        if df == 0 and ds == 0:
            for j in range(1, first):
                to_peer(phase, k + j * major).start()
        if ds == 0:
            for j in range(1, second):
                to_peer(phase, k + j * first * major).start()
        to_sibling(phase, k).start()

    def forward(phase, c):
        for k in range(c * chunk, (c + 1) * chunk):
            if k > 0:
                to_peer(phase, k).wait_recv()
                pass_on(phase, k)

    def arrive_sibling(phase, c):
        for k in range(c * chunk, (c + 1) * chunk):
            to_sibling(phase, k).wait_recv()

    def sent_all(phase):
        for k in range(chips):
            if k > 0:
                to_peer(phase, k).wait_send()
            to_sibling(phase, k).wait_send()

    barrier = pltpu.get_barrier_semaphore()
    for k in range(1, chips):
        pl.semaphore_signal(barrier, inc=1, device_id=device_at(*parts_of(k)), device_id_type=MESH)
    pl.semaphore_signal(barrier, inc=1, device_id=sibling, device_id_type=MESH)

    diagonal = lax.broadcasted_iota(jnp.int32, (points_ref.shape[0],) * 2, 0) == lax.broadcasted_iota(
        jnp.int32, (points_ref.shape[0],) * 2, 1
    )
    length = jnp.sum(jnp.where(diagonal, length_ref[...], 0.0), axis=1, keepdims=True)
    mine = points_ref[...] / length * POINT_SCALE
    pts[0] = mine
    vec[0, 0:1, :] = targets_ref[...]
    vec[0, 1:count, :] = 2.0 * bits_ref[...].astype(jnp.float32) - 1.0

    signal = signal_ref[0]
    noise = noise_ref[0]
    c1 = signal * (1.0 / LOG2E)
    c2 = signal * (1.0 / (3.0 * LOG2E * LOG2E))
    across = right_stack(mine)

    pl.semaphore_wait(barrier, chips)
    pass_on(POINTS, 0)
    pass_on(RIGHT, 0)

    def kernel_tile(slot):
        down = left_stack(pts[slot])
        square = lax.dot_general(
            down, across, (((0,), (0,)), ((), ())), preferred_element_type=jnp.float32
        )
        square = jnp.maximum(square, 1e-30)
        w = square * lax.rsqrt(square)
        tile = (signal + c1 * w + c2 * square) * jnp.exp2(-w)
        high = tile.astype(jnp.bfloat16)
        place = pl.ds(pl.multiple_of(slot * width, width), width)
        khi[place, :] = high
        klo[place, :] = (tile - high.astype(jnp.float32)).astype(jnp.bfloat16)

    def kernel_tiles(start):
        def run(j, carry):
            kernel_tile(start + j)
            return carry

        lax.fori_loop(0, chunk, run, 0)

    for c in range(first):
        forward(POINTS, c)
    for c in range(chunks):
        kernel_tiles(c * chunk)
        forward(RIGHT, c)
        if first + c < chunks:
            forward(POINTS, first + c)
    for c in range(chunks):
        arrive_sibling(POINTS, c)
        kernel_tiles(chips + c * chunk)
    for c in range(chunks):
        arrive_sibling(RIGHT, c)

    zero = jnp.zeros((count, width), jnp.float32)

    def total(value):
        return jnp.sum(value, axis=1, keepdims=True)

    def over_blocks(step, carry):
        def run(j, carry):
            for i in range(4):
                carry = step(4 * j + i, carry)
            return carry

        return lax.fori_loop(0, devices // 4, run, carry)

    def multiply(buffer, start, blocks):
        highs, lows = [], []
        for i in range(blocks):
            value = buffer[start + i]
            high = value.astype(jnp.bfloat16)
            highs.append(high)
            lows.append((value - high.astype(jnp.float32)).astype(jnp.bfloat16))
        high = jnp.concatenate(highs, axis=1)
        both = jnp.concatenate([high, jnp.concatenate(lows, axis=1)], axis=0)
        place = pl.ds(start * width, blocks * width)
        if not isinstance(start, int):
            place = pl.ds(pl.multiple_of(start * width, blocks * width), blocks * width)
        product = jnp.dot(both, khi[place, :], preferred_element_type=jnp.float32)
        rest = jnp.dot(high, klo[place, :], preferred_element_type=jnp.float32)
        return product[:count] + (product[count:] + rest)

    group = min(8, devices)

    def right_step(j, carry):
        image, norm = carry
        for i in range(group):
            value = vec[j * group + i]
            norm = norm + value * value
        return image + multiply(vec, j * group, group), norm

    summed, norm = lax.fori_loop(0, devices // group, right_step, (zero, zero))
    norm_now = total(norm)
    of_residual = summed + noise * vec[0]
    of_direction = of_residual
    sent_all(POINTS)
    sent_all(RIGHT)

    solved = zero
    residuals = vec
    for step in range(ITERS - 1):
        phase = IMAGE0 + step
        images = buffers[phase]
        images[0] = of_direction
        pass_on(phase, 0)
        curved = zero
        product = noise * of_direction

        def consume(start, curved, product):
            for i in range(chunk):
                curved = curved + vec[start + i] * images[start + i]
            return curved, product + multiply(images, start, chunk)

        for c in range(first):
            forward(phase, c)
        for c in range(chunks):
            curved, product = consume(c * chunk, curved, product)
            if c > 0:
                arrive_sibling(phase, c - 1)
                curved, product = consume(chips + (c - 1) * chunk, curved, product)
            if first + c < chunks:
                forward(phase, first + c)
        arrive_sibling(phase, chunks - 1)
        curved, product = consume(chips + (chunks - 1) * chunk, curved, product)
        sent_all(phase)
        alpha = norm_now / total(curved)
        solved = solved + alpha * vec[0]

        def reduce_pass(j, carry):
            value = residuals[j] - alpha * images[j]
            images[j] = value
            return carry + value * value

        norm_next = total(over_blocks(reduce_pass, zero))
        beta = norm_next / norm_now
        norm_now = norm_next
        of_residual = of_residual - alpha * product
        of_direction = of_residual + beta * of_direction

        if step + 2 < ITERS:

            def turn_pass(j, carry):
                vec[j] = images[j] + beta * vec[j]
                return carry

            over_blocks(turn_pass, 0)
        else:
            vec[0] = images[0] + beta * vec[0]
        residuals = images

    part = total(vec[0] * of_direction)
    square_shape = (count, 128)
    on_diagonal = lax.broadcasted_iota(jnp.int32, square_shape, 0) == lax.broadcasted_iota(
        jnp.int32, square_shape, 1
    )
    scal[0] = jnp.sum(jnp.where(on_diagonal, part, 0.0), axis=0, keepdims=True)

    def scalar_copy(k):
        return pltpu.make_async_remote_copy(
            src_ref=scal.at[0 if k == 0 else 2],
            dst_ref=scal.at[1 if k == 0 else 2 + k],
            send_sem=send_scal.at[k],
            recv_sem=recv_scal.at[k],
            device_id=sibling if k == 0 else device_at(*parts_of(k)),
            device_id_type=MESH,
        )

    scalar_copy(0).start()
    scalar_copy(0).wait_recv()
    summed = scal[0] + scal[1]
    scal[2] = summed
    for k in range(1, chips):
        scalar_copy(k).start()
    for k in range(1, chips):
        scalar_copy(k).wait_recv()
    for k in range(1, chips):
        summed = summed + scal[2 + k]
    curved = total(jnp.where(on_diagonal, summed, 0.0))
    alpha = norm_now / curved
    solution_ref[...] = solved + alpha * vec[0]
    residual_ref[...] = residuals[0] - alpha * of_direction
    for k in range(chips):
        scalar_copy(k).wait_send()


def solution(mesh):
    rows, cols = mesh.shape["row"], mesh.shape["col"]
    devices = rows * cols
    chips = devices // 2

    def body(points, lengthscale, signal, noise, targets, probe_bits):
        dims, width = points.shape
        count = probe_bits.shape[0] + 1
        block = jax.ShapeDtypeStruct((count, width), jnp.float32)
        vmem = pl.BlockSpec(memory_space=pltpu.VMEM)
        smem = pl.BlockSpec(memory_space=pltpu.SMEM)
        slots = pltpu.VMEM((devices, count, width), jnp.float32)
        return pl.pallas_call(
            functools.partial(kernel_body, rows, cols),
            out_shape=(block, block),
            in_specs=[vmem, vmem, smem, smem, vmem, vmem],
            out_specs=(vmem, vmem),
            scratch_shapes=[
                pltpu.VMEM((devices, dims, width), jnp.float32),
                slots,
                slots,
                slots,
                pltpu.VMEM((devices * width, width), jnp.bfloat16),
                pltpu.VMEM((devices * width, width), jnp.bfloat16),
                pltpu.VMEM((chips + 2, 1, 128), jnp.float32),
                pltpu.SemaphoreType.DMA((4, chips)),
                pltpu.SemaphoreType.DMA((4, chips)),
                pltpu.SemaphoreType.DMA((4, chips)),
                pltpu.SemaphoreType.DMA((4, chips)),
                pltpu.SemaphoreType.DMA((chips,)),
                pltpu.SemaphoreType.DMA((chips,)),
            ],
            compiler_params=pltpu.CompilerParams(
                collective_id=0, has_side_effects=True, vmem_limit_bytes=60 * 1024 * 1024
            ),
        )(points, lengthscale[None, :], signal, noise, targets[None, :], probe_bits)

    split_points = P(None, ("row", "col"))
    return jax.shard_map(
        body,
        mesh=mesh,
        in_specs=(split_points, P(), P(), P(), P(("row", "col")), split_points),
        out_specs=(split_points, split_points),
        check_vma=False,
    )
```

```python
import functools
import math

import jax
import jax.numpy as jnp
from jax import lax
from jax.experimental import pallas as pl
from jax.experimental.pallas import tpu as pltpu
from jax.sharding import PartitionSpec as P

ITERS = 3
MESH = pl.DeviceIdType.MESH
LOG2E = math.log2(math.e)
POINT_SCALE = math.sqrt(5.0) * LOG2E
POINTS, RIGHT, IMAGE0, IMAGE1 = range(4)


def split(value, count):
    parts = []
    for _ in range(count):
        part = value.astype(jnp.bfloat16)
        parts.append(part)
        value = value - part.astype(jnp.float32)
    return parts


def norm_rows(points, first):
    norm = jnp.sum(points * points, axis=0, keepdims=True)
    n1, n2, n3 = [part.astype(jnp.float32) for part in split(norm, 3)]
    row = lax.broadcasted_iota(jnp.int32, points.shape, 0)
    base = 0 if first else 3
    ones = 3 - base
    rows = jnp.where((row >= ones) & (row < ones + 3), 1.0, 0.0)
    for place, part in enumerate((n1, n2, n3)):
        rows = jnp.where(row == base + place, part, rows)
    return rows.astype(jnp.bfloat16)


def left_stack(points):
    s1, s2, s3 = split(points, 3)
    return jnp.concatenate([s1, s1, s2, s2, s1, s3, norm_rows(points, True)], axis=0)


def right_stack(points):
    s1, s2, s3 = split(-2.0 * points, 3)
    return jnp.concatenate([s1, s2, s1, s2, s3, s1, norm_rows(points, False)], axis=0)


def kernel_body(
    rows, cols,
    points_ref, length_ref, signal_ref, noise_ref, targets_ref, bits_ref,
    solution_ref, residual_ref,
    pts, vec, im0, im1, khi, klo, scal,
    send_peer, recv_peer, send_sib, recv_sib, send_scal, recv_scal,
):
    devices = rows * cols
    chips = devices // 2
    width = points_ref.shape[1]
    count = bits_ref.shape[0] + 1
    wide = rows // 2
    minor = 1
    while 4 * minor * minor <= cols:
        minor *= 2
    major = cols // minor
    chunk = major
    chunks = chips // chunk
    row = lax.axis_index("row")
    col = lax.axis_index("col")
    core = lax.rem(row, 2)
    x = lax.div(row, 2)
    z = lax.div(col, minor)
    y = lax.rem(col, minor)
    turned = core if wide == minor else 0
    first, second = wide, minor
    buffers = (pts, vec, im0, im1)

    def parts_of(k):
        return k % major, k // major % first, k // major // first

    def device_at(dz, df, ds):
        tx = lax.rem(x + df + turned * (ds - df), wide)
        ty = lax.rem(y + ds + turned * (df - ds), minor)
        tz = lax.rem(z + dz, major)
        return (2 * tx + core, tz * minor + ty)

    sibling = (row + 1 - 2 * core, col)

    def to_peer(phase, k):
        dz, df, ds = parts_of(k)
        if ds > 0:
            held, target = k - ds * first * major, (0, 0, ds)
        elif df > 0:
            held, target = dz, (0, df, 0)
        else:
            held, target = 0, (dz, 0, 0)
        return pltpu.make_async_remote_copy(
            src_ref=buffers[phase].at[held],
            dst_ref=buffers[phase].at[k],
            send_sem=send_peer.at[phase, k],
            recv_sem=recv_peer.at[phase, k],
            device_id=device_at(*target),
            device_id_type=MESH,
        )

    def to_sibling(phase, k):
        return pltpu.make_async_remote_copy(
            src_ref=buffers[phase].at[k],
            dst_ref=buffers[phase].at[chips + k],
            send_sem=send_sib.at[phase, k],
            recv_sem=recv_sib.at[phase, k],
            device_id=sibling,
            device_id_type=MESH,
        )

    def pass_on(phase, k):
        dz, df, ds = parts_of(k)
        if k == 0:
            for j in range(1, major):
                to_peer(phase, j).start()
        if df == 0 and ds == 0:
            for j in range(1, first):
                to_peer(phase, k + j * major).start()
        if ds == 0:
            for j in range(1, second):
                to_peer(phase, k + j * first * major).start()
        to_sibling(phase, k).start()

    def forward(phase, c):
        for k in range(c * chunk, (c + 1) * chunk):
            if k > 0:
                to_peer(phase, k).wait_recv()
                pass_on(phase, k)

    def arrive_sibling(phase, c):
        for k in range(c * chunk, (c + 1) * chunk):
            to_sibling(phase, k).wait_recv()

    def sent_all(phase):
        for k in range(chips):
            if k > 0:
                to_peer(phase, k).wait_send()
            to_sibling(phase, k).wait_send()

    barrier = pltpu.get_barrier_semaphore()
    for k in range(1, chips):
        pl.semaphore_signal(barrier, inc=1, device_id=device_at(*parts_of(k)), device_id_type=MESH)
    pl.semaphore_signal(barrier, inc=1, device_id=sibling, device_id_type=MESH)

    diagonal = lax.broadcasted_iota(jnp.int32, (points_ref.shape[0],) * 2, 0) == lax.broadcasted_iota(
        jnp.int32, (points_ref.shape[0],) * 2, 1
    )
    length = jnp.sum(jnp.where(diagonal, length_ref[...], 0.0), axis=1, keepdims=True)
    mine = points_ref[...] / length * POINT_SCALE
    pts[0] = mine
    vec[0, 0:1, :] = targets_ref[...]
    vec[0, 1:count, :] = 2.0 * bits_ref[...].astype(jnp.float32) - 1.0

    signal = signal_ref[0]
    noise = noise_ref[0]
    c1 = signal * (1.0 / LOG2E)
    c2 = signal * (1.0 / (3.0 * LOG2E * LOG2E))
    across = right_stack(mine)

    pl.semaphore_wait(barrier, chips)
    pass_on(POINTS, 0)
    pass_on(RIGHT, 0)

    def kernel_tile(slot):
        down = left_stack(pts[slot])
        square = lax.dot_general(
            down, across, (((0,), (0,)), ((), ())), preferred_element_type=jnp.float32
        )
        square = jnp.maximum(square, 1e-30)
        w = square * lax.rsqrt(square)
        tile = (signal + c1 * w + c2 * square) * jnp.exp2(-w)
        high = tile.astype(jnp.bfloat16)
        place = pl.ds(pl.multiple_of(slot * width, width), width)
        khi[place, :] = high
        klo[place, :] = (tile - high.astype(jnp.float32)).astype(jnp.bfloat16)

    def kernel_tiles(start):
        def run(j, carry):
            kernel_tile(start + 2 * j)
            kernel_tile(start + 2 * j + 1)
            return carry

        lax.fori_loop(0, chunk // 2, run, 0)
        if chunk % 2:
            kernel_tile(start + chunk - 1)

    forward(POINTS, 0)
    for c in range(chunks):
        kernel_tiles(c * chunk)
        if c + 1 < chunks:
            forward(POINTS, c + 1)
        forward(RIGHT, c)
    for c in range(chunks):
        arrive_sibling(POINTS, c)
        kernel_tiles(chips + c * chunk)
    for c in range(chunks):
        arrive_sibling(RIGHT, c)

    zero = jnp.zeros((count, width), jnp.float32)

    def total(value):
        return jnp.sum(value, axis=1, keepdims=True)

    def over_blocks(step, carry):
        def run(j, carry):
            for i in range(4):
                carry = step(4 * j + i, carry)
            return carry

        return lax.fori_loop(0, devices // 4, run, carry)

    def multiply(buffer, start, blocks):
        highs, lows = [], []
        for i in range(blocks):
            value = buffer[start + i]
            high = value.astype(jnp.bfloat16)
            highs.append(high)
            lows.append((value - high.astype(jnp.float32)).astype(jnp.bfloat16))
        high = jnp.concatenate(highs, axis=1)
        both = jnp.concatenate([high, jnp.concatenate(lows, axis=1)], axis=0)
        place = pl.ds(start * width, blocks * width)
        if not isinstance(start, int):
            place = pl.ds(pl.multiple_of(start * width, blocks * width), blocks * width)
        product = jnp.dot(both, khi[place, :], preferred_element_type=jnp.float32)
        rest = jnp.dot(high, klo[place, :], preferred_element_type=jnp.float32)
        return product[:count] + (product[count:] + rest)

    group = min(8, devices)

    def right_step(j, carry):
        image, norm = carry
        for i in range(group):
            value = vec[j * group + i]
            norm = norm + value * value
        return image + multiply(vec, j * group, group), norm

    summed, norm = lax.fori_loop(0, devices // group, right_step, (zero, zero))
    norm_now = total(norm)
    of_residual = summed + noise * vec[0]
    of_direction = of_residual

    solved = zero
    residuals = vec
    for step in range(ITERS - 1):
        phase = IMAGE0 + step
        images = buffers[phase]
        images[0] = of_direction
        pass_on(phase, 0)
        if step == 0:
            sent_all(POINTS)
            sent_all(RIGHT)
        curved = zero
        product = noise * of_direction

        def consume(start, curved, product):
            for i in range(chunk):
                curved = curved + vec[start + i] * images[start + i]
            return curved, product + multiply(images, start, chunk)

        for c in range(first):
            forward(phase, c)
        for c in range(chunks):
            curved, product = consume(c * chunk, curved, product)
            if c > 0:
                arrive_sibling(phase, c - 1)
                curved, product = consume(chips + (c - 1) * chunk, curved, product)
            if first + c < chunks:
                forward(phase, first + c)
        sent_all(phase)
        arrive_sibling(phase, chunks - 1)
        curved, product = consume(chips + (chunks - 1) * chunk, curved, product)
        alpha = norm_now / total(curved)
        solved = solved + alpha * vec[0]

        def reduce_pass(j, carry):
            value = residuals[j] - alpha * images[j]
            images[j] = value
            return carry + value * value

        norm_next = total(over_blocks(reduce_pass, zero))
        beta = norm_next / norm_now
        norm_now = norm_next
        of_residual = of_residual - alpha * product
        of_direction = of_residual + beta * of_direction

        if step + 2 < ITERS:

            def turn_pass(j, carry):
                vec[j] = images[j] + beta * vec[j]
                return carry

            over_blocks(turn_pass, 0)
        else:
            vec[0] = images[0] + beta * vec[0]
        residuals = images

    part = total(vec[0] * of_direction)
    square_shape = (count, 128)
    on_diagonal = lax.broadcasted_iota(jnp.int32, square_shape, 0) == lax.broadcasted_iota(
        jnp.int32, square_shape, 1
    )
    scal[0] = jnp.sum(jnp.where(on_diagonal, part, 0.0), axis=0, keepdims=True)

    def scalar_copy(k):
        return pltpu.make_async_remote_copy(
            src_ref=scal.at[0 if k == 0 else 2],
            dst_ref=scal.at[1 if k == 0 else 2 + k],
            send_sem=send_scal.at[k],
            recv_sem=recv_scal.at[k],
            device_id=sibling if k == 0 else device_at(*parts_of(k)),
            device_id_type=MESH,
        )

    scalar_copy(0).start()
    scalar_copy(0).wait_recv()
    summed = scal[0] + scal[1]
    scal[2] = summed
    for k in range(1, chips):
        scalar_copy(k).start()
    for k in range(1, chips):
        scalar_copy(k).wait_recv()
    for k in range(1, chips):
        summed = summed + scal[2 + k]
    curved = total(jnp.where(on_diagonal, summed, 0.0))
    alpha = norm_now / curved
    solution_ref[...] = solved + alpha * vec[0]
    residual_ref[...] = residuals[0] - alpha * of_direction
    for k in range(chips):
        scalar_copy(k).wait_send()


def solution(mesh):
    rows, cols = mesh.shape["row"], mesh.shape["col"]
    devices = rows * cols
    chips = devices // 2

    def body(points, lengthscale, signal, noise, targets, probe_bits):
        dims, width = points.shape
        count = probe_bits.shape[0] + 1
        block = jax.ShapeDtypeStruct((count, width), jnp.float32)
        vmem = pl.BlockSpec(memory_space=pltpu.VMEM)
        smem = pl.BlockSpec(memory_space=pltpu.SMEM)
        slots = pltpu.VMEM((devices, count, width), jnp.float32)
        return pl.pallas_call(
            functools.partial(kernel_body, rows, cols),
            out_shape=(block, block),
            in_specs=[vmem, vmem, smem, smem, vmem, vmem],
            out_specs=(vmem, vmem),
            scratch_shapes=[
                pltpu.VMEM((devices, dims, width), jnp.float32),
                slots,
                slots,
                slots,
                pltpu.VMEM((devices * width, width), jnp.bfloat16),
                pltpu.VMEM((devices * width, width), jnp.bfloat16),
                pltpu.VMEM((chips + 2, 1, 128), jnp.float32),
                pltpu.SemaphoreType.DMA((4, chips)),
                pltpu.SemaphoreType.DMA((4, chips)),
                pltpu.SemaphoreType.DMA((4, chips)),
                pltpu.SemaphoreType.DMA((4, chips)),
                pltpu.SemaphoreType.DMA((chips,)),
                pltpu.SemaphoreType.DMA((chips,)),
            ],
            compiler_params=pltpu.CompilerParams(
                collective_id=0, has_side_effects=True, vmem_limit_bytes=60 * 1024 * 1024
            ),
        )(points, lengthscale[None, :], signal, noise, targets[None, :], probe_bits)

    split_points = P(None, ("row", "col"))
    return jax.shard_map(
        body,
        mesh=mesh,
        in_specs=(split_points, P(), P(), P(), P(("row", "col")), split_points),
        out_specs=(split_points, split_points),
        check_vma=False,
    )
```

```python
import functools
import math

import jax
import jax.numpy as jnp
from jax import lax
from jax.experimental import pallas as pl
from jax.experimental.pallas import tpu as pltpu
from jax.sharding import PartitionSpec as P

ITERS = 3
MESH = pl.DeviceIdType.MESH
LOG2E = math.log2(math.e)
POINT_SCALE = math.sqrt(5.0) * LOG2E
POINTS, RIGHT, IMAGE0, IMAGE1 = range(4)


def split(value, count):
    parts = []
    for _ in range(count):
        part = value.astype(jnp.bfloat16)
        parts.append(part)
        value = value - part.astype(jnp.float32)
    return parts


def norm_rows(points, first):
    norm = jnp.sum(points * points, axis=0, keepdims=True)
    n1, n2, n3 = [part.astype(jnp.float32) for part in split(norm, 3)]
    row = lax.broadcasted_iota(jnp.int32, points.shape, 0)
    base = 0 if first else 3
    ones = 3 - base
    rows = jnp.where((row >= ones) & (row < ones + 3), 1.0, 0.0)
    for place, part in enumerate((n1, n2, n3)):
        rows = jnp.where(row == base + place, part, rows)
    return rows.astype(jnp.bfloat16)


def left_stack(points):
    s1, s2, s3 = split(points, 3)
    return jnp.concatenate([s1, s1, s2, s2, s1, s3, norm_rows(points, True)], axis=0)


def right_stack(points):
    s1, s2, s3 = split(-2.0 * points, 3)
    return jnp.concatenate([s1, s2, s1, s2, s3, s1, norm_rows(points, False)], axis=0)


def kernel_body(
    rows, cols,
    points_ref, length_ref, signal_ref, noise_ref, targets_ref, bits_ref,
    solution_ref, residual_ref,
    pts, vec, im0, im1, khi, klo, scal,
    send_peer, recv_peer, send_sib, recv_sib, send_scal, recv_scal,
):
    devices = rows * cols
    chips = devices // 2
    width = points_ref.shape[1]
    count = bits_ref.shape[0] + 1
    wide = rows // 2
    minor = 1
    while 4 * minor * minor <= cols:
        minor *= 2
    major = cols // minor
    chunk = major
    chunks = chips // chunk
    row = lax.axis_index("row")
    col = lax.axis_index("col")
    core = lax.rem(row, 2)
    x = lax.div(row, 2)
    z = lax.div(col, minor)
    y = lax.rem(col, minor)
    turned = core if wide == minor else 0
    first, second = wide, minor
    buffers = (pts, vec, im0, im1)

    def parts_of(k):
        return k % major, k // major % first, k // major // first

    def device_at(dz, df, ds):
        tx = lax.rem(x + df + turned * (ds - df), wide)
        ty = lax.rem(y + ds + turned * (df - ds), minor)
        tz = lax.rem(z + dz, major)
        return (2 * tx + core, tz * minor + ty)

    sibling = (row + 1 - 2 * core, col)

    def to_peer(phase, k):
        dz, df, ds = parts_of(k)
        if ds > 0:
            held, target = k - ds * first * major, (0, 0, ds)
        elif df > 0:
            held, target = dz, (0, df, 0)
        else:
            held, target = 0, (dz, 0, 0)
        return pltpu.make_async_remote_copy(
            src_ref=buffers[phase].at[held],
            dst_ref=buffers[phase].at[k],
            send_sem=send_peer.at[phase, k],
            recv_sem=recv_peer.at[phase, k],
            device_id=device_at(*target),
            device_id_type=MESH,
        )

    def to_sibling(phase, k):
        return pltpu.make_async_remote_copy(
            src_ref=buffers[phase].at[k],
            dst_ref=buffers[phase].at[chips + k],
            send_sem=send_sib.at[phase, k],
            recv_sem=recv_sib.at[phase, k],
            device_id=sibling,
            device_id_type=MESH,
        )

    def pass_on(phase, k):
        dz, df, ds = parts_of(k)
        if k == 0:
            for j in range(1, major):
                to_peer(phase, j).start()
        if df == 0 and ds == 0:
            for j in range(1, first):
                to_peer(phase, k + j * major).start()
        if ds == 0:
            for j in range(1, second):
                to_peer(phase, k + j * first * major).start()
        to_sibling(phase, k).start()

    def forward(phase, c):
        for k in range(c * chunk, (c + 1) * chunk):
            if k > 0:
                to_peer(phase, k).wait_recv()
                pass_on(phase, k)

    def arrive_sibling(phase, c):
        for k in range(c * chunk, (c + 1) * chunk):
            to_sibling(phase, k).wait_recv()

    def sent_all(phase):
        for k in range(chips):
            if k > 0:
                to_peer(phase, k).wait_send()
            to_sibling(phase, k).wait_send()

    barrier = pltpu.get_barrier_semaphore()
    for k in range(1, chips):
        pl.semaphore_signal(barrier, inc=1, device_id=device_at(*parts_of(k)), device_id_type=MESH)
    pl.semaphore_signal(barrier, inc=1, device_id=sibling, device_id_type=MESH)

    diagonal = lax.broadcasted_iota(jnp.int32, (points_ref.shape[0],) * 2, 0) == lax.broadcasted_iota(
        jnp.int32, (points_ref.shape[0],) * 2, 1
    )
    length = jnp.sum(jnp.where(diagonal, length_ref[...], 0.0), axis=1, keepdims=True)
    mine = points_ref[...] / length * POINT_SCALE
    pts[0] = mine
    vec[0, 0:1, :] = targets_ref[...]
    vec[0, 1:count, :] = 2.0 * bits_ref[...].astype(jnp.float32) - 1.0

    signal = signal_ref[0]
    noise = noise_ref[0]
    c1 = signal * (1.0 / LOG2E)
    c2 = signal * (1.0 / (3.0 * LOG2E * LOG2E))
    across = right_stack(mine)

    def kernel_tile(slot):
        down = left_stack(pts[slot])
        square = lax.dot_general(
            down, across, (((0,), (0,)), ((), ())), preferred_element_type=jnp.float32
        )
        square = jnp.maximum(square, 1e-30)
        w = square * lax.rsqrt(square)
        tile = (signal + c1 * w + c2 * square) * jnp.exp2(-w)
        high = tile.astype(jnp.bfloat16)
        place = pl.ds(pl.multiple_of(slot * width, width), width)
        khi[place, :] = high
        klo[place, :] = (tile - high.astype(jnp.float32)).astype(jnp.bfloat16)

    def kernel_tiles(start):
        def run(j, carry):
            kernel_tile(start + 2 * j)
            kernel_tile(start + 2 * j + 1)
            return carry

        lax.fori_loop(0, chunk // 2, run, 0)
        if chunk % 2:
            kernel_tile(start + chunk - 1)

    kernel_tile(0)
    pl.semaphore_wait(barrier, chips)
    pass_on(POINTS, 0)
    pass_on(RIGHT, 0)

    forward(POINTS, 0)
    for c in range(chunks):
        if c == 0:
            for k in range(1, chunk):
                kernel_tile(k)
        else:
            kernel_tiles(c * chunk)
        if c + 1 < chunks:
            forward(POINTS, c + 1)
        forward(RIGHT, c)
    for c in range(chunks):
        arrive_sibling(POINTS, c)
        kernel_tiles(chips + c * chunk)
    for c in range(chunks):
        arrive_sibling(RIGHT, c)

    zero = jnp.zeros((count, width), jnp.float32)

    def total(value):
        return jnp.sum(value, axis=1, keepdims=True)

    def over_blocks(step, carry):
        def run(j, carry):
            for i in range(4):
                carry = step(4 * j + i, carry)
            return carry

        return lax.fori_loop(0, devices // 4, run, carry)

    def multiply(buffer, start, blocks):
        highs, lows = [], []
        for i in range(blocks):
            value = buffer[start + i]
            high = value.astype(jnp.bfloat16)
            highs.append(high)
            lows.append((value - high.astype(jnp.float32)).astype(jnp.bfloat16))
        high = jnp.concatenate(highs, axis=1)
        both = jnp.concatenate([high, jnp.concatenate(lows, axis=1)], axis=0)
        place = pl.ds(start * width, blocks * width)
        if not isinstance(start, int):
            place = pl.ds(pl.multiple_of(start * width, blocks * width), blocks * width)
        product = jnp.dot(both, khi[place, :], preferred_element_type=jnp.float32)
        rest = jnp.dot(high, klo[place, :], preferred_element_type=jnp.float32)
        return product[:count] + (product[count:] + rest)

    group = min(8, devices)

    def right_step(j, carry):
        image, norm = carry
        for i in range(group):
            value = vec[j * group + i]
            norm = norm + value * value
        return image + multiply(vec, j * group, group), norm

    summed, norm = lax.fori_loop(0, devices // group, right_step, (zero, zero))
    norm_now = total(norm)
    of_residual = summed + noise * vec[0]
    of_direction = of_residual

    solved = zero
    residuals = vec
    for step in range(ITERS - 1):
        phase = IMAGE0 + step
        images = buffers[phase]
        images[0] = of_direction
        pass_on(phase, 0)
        if step == 0:
            sent_all(POINTS)
            sent_all(RIGHT)
        curved = zero
        product = noise * of_direction

        def consume(start, curved, product):
            for i in range(chunk):
                curved = curved + vec[start + i] * images[start + i]
            return curved, product + multiply(images, start, chunk)

        for c in range(first):
            forward(phase, c)
        for c in range(chunks):
            curved, product = consume(c * chunk, curved, product)
            if c > 0:
                arrive_sibling(phase, c - 1)
                curved, product = consume(chips + (c - 1) * chunk, curved, product)
            if first + c < chunks:
                forward(phase, first + c)
        sent_all(phase)
        arrive_sibling(phase, chunks - 1)
        curved, product = consume(chips + (chunks - 1) * chunk, curved, product)
        alpha = norm_now / total(curved)
        solved = solved + alpha * vec[0]

        def reduce_pass(j, carry):
            value = residuals[j] - alpha * images[j]
            images[j] = value
            return carry + value * value

        norm_next = total(over_blocks(reduce_pass, zero))
        beta = norm_next / norm_now
        norm_now = norm_next
        of_residual = of_residual - alpha * product
        of_direction = of_residual + beta * of_direction

        if step + 2 < ITERS:

            def turn_pass(j, carry):
                vec[j] = images[j] + beta * vec[j]
                return carry

            over_blocks(turn_pass, 0)
        else:
            vec[0] = images[0] + beta * vec[0]
        residuals = images

    part = total(vec[0] * of_direction)
    square_shape = (count, 128)
    on_diagonal = lax.broadcasted_iota(jnp.int32, square_shape, 0) == lax.broadcasted_iota(
        jnp.int32, square_shape, 1
    )
    scal[0] = jnp.sum(jnp.where(on_diagonal, part, 0.0), axis=0, keepdims=True)

    def scalar_copy(k):
        return pltpu.make_async_remote_copy(
            src_ref=scal.at[0 if k == 0 else 2],
            dst_ref=scal.at[1 if k == 0 else 2 + k],
            send_sem=send_scal.at[k],
            recv_sem=recv_scal.at[k],
            device_id=sibling if k == 0 else device_at(*parts_of(k)),
            device_id_type=MESH,
        )

    scalar_copy(0).start()
    scalar_copy(0).wait_recv()
    summed = scal[0] + scal[1]
    scal[2] = summed
    for k in range(1, chips):
        scalar_copy(k).start()
    for k in range(1, chips):
        scalar_copy(k).wait_recv()
    for k in range(1, chips):
        summed = summed + scal[2 + k]
    curved = total(jnp.where(on_diagonal, summed, 0.0))
    alpha = norm_now / curved
    solution_ref[...] = solved + alpha * vec[0]
    residual_ref[...] = residuals[0] - alpha * of_direction
    for k in range(chips):
        scalar_copy(k).wait_send()


def solution(mesh):
    rows, cols = mesh.shape["row"], mesh.shape["col"]
    devices = rows * cols
    chips = devices // 2

    def body(points, lengthscale, signal, noise, targets, probe_bits):
        dims, width = points.shape
        count = probe_bits.shape[0] + 1
        block = jax.ShapeDtypeStruct((count, width), jnp.float32)
        vmem = pl.BlockSpec(memory_space=pltpu.VMEM)
        smem = pl.BlockSpec(memory_space=pltpu.SMEM)
        slots = pltpu.VMEM((devices, count, width), jnp.float32)
        return pl.pallas_call(
            functools.partial(kernel_body, rows, cols),
            out_shape=(block, block),
            in_specs=[vmem, vmem, smem, smem, vmem, vmem],
            out_specs=(vmem, vmem),
            scratch_shapes=[
                pltpu.VMEM((devices, dims, width), jnp.float32),
                slots,
                slots,
                slots,
                pltpu.VMEM((devices * width, width), jnp.bfloat16),
                pltpu.VMEM((devices * width, width), jnp.bfloat16),
                pltpu.VMEM((chips + 2, 1, 128), jnp.float32),
                pltpu.SemaphoreType.DMA((4, chips)),
                pltpu.SemaphoreType.DMA((4, chips)),
                pltpu.SemaphoreType.DMA((4, chips)),
                pltpu.SemaphoreType.DMA((4, chips)),
                pltpu.SemaphoreType.DMA((chips,)),
                pltpu.SemaphoreType.DMA((chips,)),
            ],
            compiler_params=pltpu.CompilerParams(
                collective_id=0, has_side_effects=True, vmem_limit_bytes=60 * 1024 * 1024
            ),
        )(points, lengthscale[None, :], signal, noise, targets[None, :], probe_bits)

    split_points = P(None, ("row", "col"))
    return jax.shard_map(
        body,
        mesh=mesh,
        in_specs=(split_points, P(), P(), P(), P(("row", "col")), split_points),
        out_specs=(split_points, split_points),
        check_vma=False,
    )
```
